32 devices in a mesh: space: 8 (over z, y), slab: 4 (over x, core).
Axes of the slice: x: 2, y: 2, z: 4, core: 2. Of those that a mesh axis runs over, the one named last changes fastest.
Arguments:
- source: float32 [4, 256, 2048], P('slab', None, 'space'), may hold values from -6 to 6
- initial: float32 [64, 2048], P(None, 'space'), may hold values from -6 to 6
- inverse: float32 [256, 256], replicated, may hold values from -0.1 to 0.7, as said below
- lift: float32 [256, 384], replicated, may hold values from -0.109375 to 0.109375
- lift_time: float32 [256, 64], replicated, may hold values from -0.375 to 0.375
- links: int32 [6, 2048], P(None, 'space'), may hold values from 0 to 1791, as said below
- orient: int32 [6, 2048], P(None, 'space'), may hold values from 0 to 7
- exports: int32 [2048], P('space'), may hold values from 0 to 1535, as said below
- counts: int32 [8], P('space'), may hold values from 128 to 256, as said below
Outputs:
- state: float32 [4, 256, 2048], P('slab', None, 'space')
The draws below stay inside these ranges and needn't reach their ends.
Inputs may be any that keep to these rules, and one draw needn't show every extreme that they name: `links`: a value below 1536 is f*256 + e naming face f of a live slot e of the same partition; others are 1536 + m naming slot m of the imported neighbour traces. `exports`: each value is f*256 + e with e a live slot of that partition. `counts`: some partition holds exactly 256. `inverse`: full rank; diagonal entries between 0.5 and 0.7, off-diagonal entries of magnitude at most 0.1.
All inputs are finite; a program needn't handle non-finite values.
Results may differ from the reference program's by a relative error of at most 0.0001.
Values sent between devices are 32-bit elements; how exact they have to be, the bound alone decides.
No kernel may reach another device: no remote copies, remote signals or barrier semaphores. Data moves between devices by JAX's collectives and lax.ppermute only.
A program may use at most 64 MiB of HBM per device.

```python
import jax
import jax.numpy as jnp
from jax import lax

ELEM_DEV = 256
ITERS = 6
PEER_CAP = 128
ELEMS = 2048
N_SPACE = 8
N_SLAB = 4


def counts_of(key):
    base = jax.random.fold_in(key, 101)
    values = jax.random.randint(base, (N_SPACE,), ELEM_DEV // 2, ELEM_DEV + 1)
    fullest = jax.random.randint(jax.random.fold_in(base, 1), (), 0, N_SPACE)
    return jnp.where(jnp.arange(N_SPACE) == fullest, ELEM_DEV, values).astype(jnp.int32)


def draw_counts(key, part):
    return counts_of(key)


def draw_links(key, part):
    live = jnp.repeat(counts_of(key), ELEM_DEV)
    keys = jax.random.split(jax.random.fold_in(key, 202), 4)
    shape = (6, ELEM_DEV * N_SPACE)
    element = jax.random.randint(keys[0], shape, 0, jnp.broadcast_to(live[None, :], shape))
    facing = jax.random.randint(keys[1], shape, 0, 6)
    remote = jax.random.randint(keys[2], shape, 0, 2 * PEER_CAP)
    crossing = jax.random.randint(keys[3], shape, 0, 4) == 0
    return jnp.where(crossing, 6 * ELEM_DEV + remote, facing * ELEM_DEV + element).astype(jnp.int32)


def draw_exports(key, part):
    live = jnp.repeat(counts_of(key), 2 * PEER_CAP)
    keys = jax.random.split(jax.random.fold_in(key, 303), 2)
    shape = (2 * PEER_CAP * N_SPACE,)
    element = jax.random.randint(keys[0], shape, 0, live)
    facing = jax.random.randint(keys[1], shape, 0, 6)
    return (facing * ELEM_DEV + element).astype(jnp.int32)


def draw_inverse(key, part):
    noise = jnp.clip(jax.random.normal(key, (256, 256), jnp.float32), -4.0, 4.0)
    return 0.6 * jnp.eye(256, dtype=jnp.float32) + 0.025 * noise


def plant(array, rng, low, largest):
    shape = array.shape
    index_at = [jax.random.randint(jax.random.fold_in(rng, axis), (), 0, shape[axis]) for axis in range(len(shape))]
    array = array.at[tuple(index_at)].set(low)
    longest = shape.index(max(shape))
    index_at[longest] = (index_at[longest] + 1) % shape[longest]
    return array.at[tuple(index_at)].set(largest)


def level_of(key, dims, shards, smallest, largest):
    factor_of, own = 1.0, jax.random.fold_in(key, 6)
    for axis_at, blocks in shards:
        steps = jnp.exp(jax.random.uniform(jax.random.fold_in(own, axis_at), (blocks,), jnp.float32, smallest / len(shards), largest / len(shards)))
        factor_of = factor_of * jnp.repeat(steps, dims[axis_at] // blocks).reshape([-1 if axis == axis_at else 1 for axis in range(len(dims))])
    return factor_of


def bell_draw(own_key, dims, width, limit, cuts=(), kind=jnp.bfloat16):
    result = width * jax.random.normal(own_key, dims, jnp.float32)
    if cuts:
        result = result * level_of(own_key, dims, cuts, -0.22, 0.18)
    return jnp.clip(result, -limit, limit).astype(kind)


def setup_inputs(seed: int = 0) -> dict:
    arg_keys = jax.random.split(jax.random.key(seed), 10)
    return {
        "source": bell_draw(arg_keys[0], (N_SLAB, 256, ELEMS), 1.0, 6.0, ((0, 4), (2, 8)), jnp.float32),
        "initial": bell_draw(arg_keys[1], (64, ELEMS), 1.0, 6.0, ((1, 8),), jnp.float32),
        "inverse": draw_inverse(jax.random.fold_in(arg_keys[9], 71), 0),
        "lift": bell_draw(arg_keys[3], (256, 384), 3072 ** -0.5, 0.109375, (), jnp.float32),
        "lift_time": bell_draw(arg_keys[4], (256, 64), 256 ** -0.5, 0.375, (), jnp.float32),
        "links": draw_links(jax.random.fold_in(arg_keys[9], 71), 0),
        "orient": plant(jax.random.randint(arg_keys[6], (6, ELEMS), 0, 8), jax.random.fold_in(arg_keys[6], 1), 0, 7).astype(jnp.int32),
        "exports": draw_exports(jax.random.fold_in(arg_keys[9], 71), 0),
        "counts": draw_counts(jax.random.fold_in(arg_keys[9], 71), 0),
    }


def face_stack(volume, axis):
    pieces = [volume[:, 0], volume[:, 3], volume[:, :, 0], volume[:, :, 3], volume[:, :, :, 0], volume[:, :, :, 3]]
    return jnp.stack(pieces, axis=axis)


def orient_traces(values, turn):
    swapped = jnp.swapaxes(values, 1, 2)
    values = jnp.where(jnp.bitwise_and(turn, 4) > 0, swapped, values)
    values = jnp.where(jnp.bitwise_and(turn, 1) > 0, jnp.flip(values, 1), values)
    values = jnp.where(jnp.bitwise_and(turn, 2) > 0, jnp.flip(values, 2), values)
    return values


def reference(source, initial, inverse, lift, lift_time, links, orient, exports, counts):
    highest = lax.Precision.HIGHEST
    parts = N_SPACE
    elems = ELEM_DEV
    peer = PEER_CAP
    live = (jnp.arange(elems, dtype=jnp.int32)[None, :] < counts[:, None]).astype(jnp.float32).reshape(1, parts * elems)
    index = links.reshape(6, parts, elems).transpose(1, 0, 2).reshape(parts, 6 * elems)
    turn = orient.reshape(6, parts, elems).transpose(1, 0, 2)
    outgo = exports.reshape(parts, 2 * peer)
    lift_three = lift.reshape(256, 64, 6)
    state = jnp.zeros((N_SLAB, 256, parts * elems), jnp.float32)
    for step in range(ITERS):
        fresh = []
        for slab in range(N_SLAB):
            volume = state[slab].reshape(4, 4, 4, 4, parts, elems)
            traces = face_stack(volume, 4).reshape(64, parts, 6 * elems)
            sent = jnp.take_along_axis(traces, outgo[None], axis=2)
            from_lower = jnp.roll(sent[:, :, peer:], 1, axis=1)
            from_upper = jnp.roll(sent[:, :, :peer], -1, axis=1)
            table = jnp.concatenate([traces, from_lower, from_upper], axis=2)
            nbr = jnp.take_along_axis(table, index[None], axis=2).reshape(4, 4, 4, parts, 6, elems)
            nbr = orient_traces(nbr, turn).reshape(64, parts, 6, elems)
            spatial = jnp.einsum('rcf,cnfe->rne', lift_three, nbr, precision=highest).reshape(256, parts * elems)
            if slab == 0:
                top = initial
            else:
                top = state[slab - 1][192:]
            rhs = source[slab] + spatial + jnp.dot(lift_time, top, precision=highest)
            fresh.append(jnp.dot(inverse, rhs, precision=highest) * live)
        state = jnp.stack(fresh)
    return state
```

```python
import jax
import jax.numpy as jnp
from jax import lax
from jax.experimental import pallas as pl
from jax.experimental.pallas import tpu as pltpu
from jax.sharding import PartitionSpec as P

ITERS = 6
F32 = jnp.float32
BF16 = jnp.bfloat16

VMEM = pl.BlockSpec(memory_space=pltpu.VMEM)
SMEM = pl.BlockSpec(memory_space=pltpu.SMEM)


def mm(a, b):
    return jnp.dot(a, b, preferred_element_type=F32)


def split(x):
    hi = x.astype(BF16)
    return hi, (x - hi.astype(F32)).astype(BF16)


def iota(shape, dim):
    return lax.broadcasted_iota(jnp.int32, shape, dim)


def one_hot(hit):
    return jnp.where(hit, 1.0, 0.0).astype(BF16)


def halves(x):
    hi = x.astype(BF16).astype(F32)
    return jnp.where(iota(x.shape, 0) % 8 < 4, hi, x - hi)


def face_node(face, a, b):
    end = 3 * (face % 2)
    if face < 2:
        return end * 16 + a * 4 + b
    if face < 4:
        return a * 16 + end * 4 + b
    return a * 16 + b * 4 + end


def publish(rows, rows_ref, exports, table_ref, top_ref, low_ref, high_ref):
    elems = rows.shape[1]
    peer = low_ref.shape[1]
    for c in range(rows_ref.shape[0]):
        rows_ref[c] = rows[:, c * 128 : (c + 1) * 128]
        top_ref[:, c * 128 : (c + 1) * 128] = rows_ref[c, pl.ds(3, 64, stride=8), :]
    parts = halves(rows)
    sent = None
    for face in range(6):
        piece = jnp.concatenate(
            [parts[8 * face_node(face, a, b) :][:8] for a in range(4) for b in range(4)], axis=0
        ).astype(BF16)
        table_ref[:, face * elems : (face + 1) * elems] = piece
    pick = one_hot(iota((6 * elems, 2 * peer), 0) == exports)
    sent = mm(table_ref[...], pick)
    first = iota((8, 2 * peer), 0) < 4
    for m in range(8):
        even = sent[16 * m : 16 * m + 8]
        odd = sent[16 * m + 8 : 16 * m + 16]
        even = even + pltpu.roll(even, 4, 0)
        odd = odd + pltpu.roll(odd, 4, 0)
        both = jnp.where(first, even, odd)
        low_ref[8 * m : 8 * m + 8, :] = both[:, :peer]
        high_ref[8 * m : 8 * m + 8, :] = both[:, peer:]


def live_of(counts_ref, elems):
    return jnp.where(iota((1, elems), 1) < counts_ref[0], 1.0, 0.0)


def prepare(counts, first, source, initial, inverse, lift, lift_time, exports,
            weight, base, table, top, low, high, rows_ref):
    elems = source.shape[2]
    dup = iota((512, 256), 0)
    row_pick = one_hot((dup % 4) * 64 + dup // 8 == iota((512, 256), 1))
    inv_hi, inv_lo = split(inverse[...])
    inv_hi = mm(row_pick, inv_hi).astype(BF16)
    inv_lo = mm(row_pick, inv_lo).astype(BF16)

    def solve(x_hi, x_lo):
        return mm(inv_hi, x_hi) + (mm(inv_hi, x_lo) + mm(inv_lo, x_hi))

    start = initial[...] * jnp.where(first[0] > 0, 1.0, 0.0)
    lt_hi, lt_lo = split(lift_time[...])
    st_hi, st_lo = split(start)
    rhs = source[0] + (mm(lt_hi, st_hi) + (mm(lt_hi, st_lo) + mm(lt_lo, st_hi)))
    rows = solve(*split(rhs)) * live_of(counts, elems)
    base[...] = rows
    publish(rows, rows_ref, exports[...], table, top, low, high)

    col = iota((384, 768), 1)
    want = ((col % 4) * 16 + (col // 8) % 16) * 6 + col // 128
    col_pick = one_hot(want == iota((384, 768), 0))
    l_hi, l_lo = split(lift[...])
    l_hi = mm(l_hi, col_pick).astype(BF16)
    l_lo = mm(l_lo, col_pick).astype(BF16)
    w_hi, w_lo = split(solve(l_hi, l_lo))
    weight[0:512, 0:768] = w_hi
    weight[512:1024, 0:768] = w_lo
    t_hi, t_lo = split(solve(jnp.concatenate([lt_hi, lt_hi], 1), jnp.concatenate([lt_lo, lt_lo], 1)))
    weight[0:512, 768:896] = t_hi
    weight[512:1024, 768:896] = t_lo


def gather_local(table, links, out):
    elems = links.shape[1] // 6
    for face in range(6):
        cols = slice(face * elems, (face + 1) * elems)
        pick = one_hot(iota((6 * elems, elems), 0) == links[:, cols])
        out[:, cols] = mm(table[...], pick).astype(BF16)


def advance(counts, local, from_low, from_high, top_in, weight, base, links, orient, nbr):
    elems = base.shape[1]
    peer = from_low.shape[1]
    first = iota((8, peer), 0) < 4
    sides = []
    for ref in (from_low, from_high):
        slabs = []
        for m in range(8):
            v = ref[8 * m : 8 * m + 8, :]
            r = pltpu.roll(v, 4, 0)
            slabs += [jnp.where(first, v, r), jnp.where(first, r, v)]
        sides.append(halves(jnp.concatenate(slabs, axis=0)).astype(BF16))
    imported = jnp.concatenate(sides, axis=1)
    for face in range(6):
        cols = slice(face * elems, (face + 1) * elems)
        pick = one_hot(iota((2 * peer, elems), 0) + 6 * elems == links[:, cols])
        got = local[:, cols].astype(F32) + mm(imported, pick)
        turn = jnp.broadcast_to(orient[:, cols], (8, elems))
        swap = (turn & 4) > 0
        rev_a = (turn & 1) > 0
        rev_b = (turn & 2) > 0
        v = [[got[8 * (a * 4 + b) :][:8] for b in range(4)] for a in range(4)]
        v = [[v[a][b] if a == b else jnp.where(swap, v[b][a], v[a][b]) for b in range(4)] for a in range(4)]
        v = [[jnp.where(rev_a, v[3 - a][b], v[a][b]) for b in range(4)] for a in range(4)]
        v = [[jnp.where(rev_b, v[a][3 - b], v[a][b]) for b in range(4)] for a in range(4)]
        nbr[face * 128 : (face + 1) * 128, :] = jnp.concatenate(sum(v, []), axis=0).astype(BF16)
    t_hi, t_lo = split(top_in[...])
    nbr[768:832, :] = t_hi
    nbr[832:896, :] = t_lo
    x = nbr[...]
    both = mm(weight[0:512, :], x) + mm(weight[512:1024, :], x)
    return (both + base[...]) * live_of(counts, elems)


def step_kernel(counts, local, from_low, from_high, top_in, weight, base, links, orient, exports,
                table, top, low, high, nbr, rows_ref):
    rows = advance(counts, local, from_low, from_high, top_in, weight, base, links, orient, nbr)
    publish(rows, rows_ref, exports[...], table, top, low, high)


def last_kernel(counts, local, from_low, from_high, top_in, weight, base, links, orient,
                out, nbr, rows_ref):
    rows = advance(counts, local, from_low, from_high, top_in, weight, base, links, orient, nbr)
    for c in range(rows_ref.shape[0]):
        rows_ref[c] = rows[:, c * 128 : (c + 1) * 128]
        for t in range(4):
            out[0, t * 64 : (t + 1) * 64, c * 128 : (c + 1) * 128] = rows_ref[c, pl.ds(t, 64, stride=8), :]


def body(source, initial, inverse, lift, lift_time, links, orient, exports, counts):
    elems = links.shape[1]
    peer = exports.shape[0] // 2
    links = links.reshape(1, 6 * elems)
    orient = orient.reshape(1, 6 * elems)
    exports = exports.reshape(1, 2 * peer)
    first = (lax.axis_index("slab") == 0).astype(jnp.int32).reshape(1)
    spaces = lax.axis_size("space")
    up = [(i, (i + 1) % spaces) for i in range(spaces)]
    down = [(b, a) for a, b in up]
    later = [(i, i + 1) for i in range(lax.axis_size("slab") - 1)]
    S = jax.ShapeDtypeStruct
    published = [
        S((128, 6 * elems), BF16),
        S((64, elems), F32),
        S((64, peer), F32),
        S((64, peer), F32),
    ]
    rows_scratch = pltpu.VMEM((elems // 128, 512, 128), F32)
    nbr_scratch = pltpu.VMEM((896, elems), BF16)

    weight, base, table, top, low, high = pl.pallas_call(
        prepare,
        out_shape=[S((1024, 896), BF16), S((512, elems), F32)] + published,
        in_specs=[SMEM, SMEM] + [VMEM] * 6,
        out_specs=[VMEM] * 6,
        scratch_shapes=[rows_scratch],
        name="prepare",
    )(counts, first, source, initial, inverse, lift, lift_time, exports)
    for step in range(1, ITERS):
        from_low = lax.ppermute(high, "space", up)
        from_high = lax.ppermute(low, "space", down)
        top_in = lax.ppermute(top, "slab", later)
        local = pl.pallas_call(
            gather_local,
            out_shape=S((128, 6 * elems), BF16),
            in_specs=[VMEM] * 2,
            out_specs=VMEM,
            name="gather_local",
        )(table, links)
        args = (counts, local, from_low, from_high, top_in, weight, base, links, orient)
        if step < ITERS - 1:
            table, top, low, high = pl.pallas_call(
                step_kernel,
                out_shape=published,
                in_specs=[SMEM] + [VMEM] * 9,
                out_specs=[VMEM] * 4,
                scratch_shapes=[nbr_scratch, rows_scratch],
                name="advance",
            )(*args, exports)
        else:
            out = pl.pallas_call(
                last_kernel,
                out_shape=S((1, 256, elems), F32),
                in_specs=[SMEM] + [VMEM] * 8,
                out_specs=VMEM,
                scratch_shapes=[nbr_scratch, rows_scratch],
                name="advance_last",
            )(*args)
    return out


def solution(mesh):
    return jax.shard_map(
        body,
        mesh=mesh,
        in_specs=(
            P("slab", None, "space"),
            P(None, "space"),
            P(),
            P(),
            P(),
            P(None, "space"),
            P(None, "space"),
            P("space"),
            P("space"),
        ),
        out_specs=P("slab", None, "space"),
        check_vma=False,
    )
```

```python
import jax
import jax.numpy as jnp
from jax import lax
from jax.experimental import pallas as pl
from jax.experimental.pallas import tpu as pltpu
from jax.sharding import PartitionSpec as P

ITERS = 6
F32 = jnp.float32
BF16 = jnp.bfloat16

VMEM = pl.BlockSpec(memory_space=pltpu.VMEM)
SMEM = pl.BlockSpec(memory_space=pltpu.SMEM)


def mm(a, b):
    return jnp.dot(a, b, preferred_element_type=F32)


def split(x):
    hi = x.astype(BF16)
    return hi, (x - hi.astype(F32)).astype(BF16)


def iota(shape, dim):
    return lax.broadcasted_iota(jnp.int32, shape, dim)


def one_hot(hit):
    return jnp.where(hit, 1.0, 0.0).astype(BF16)


def halves(x):
    hi = x.astype(BF16).astype(F32)
    return jnp.where(iota(x.shape, 0) % 8 < 4, hi, x - hi)


def face_node(face, a, b):
    end = 3 * (face % 2)
    if face < 2:
        return end * 16 + a * 4 + b
    if face < 4:
        return a * 16 + end * 4 + b
    return a * 16 + b * 4 + end


def publish(rows, rows_ref, exports, table_ref, top_ref, low_ref, high_ref):
    elems = rows.shape[1]
    peer = low_ref.shape[1]
    for c in range(rows_ref.shape[0]):
        rows_ref[c] = rows[:, c * 128 : (c + 1) * 128]
        top_ref[:, c * 128 : (c + 1) * 128] = rows_ref[c, pl.ds(3, 64, stride=8), :]
    parts = halves(rows)
    sent = None
    for face in range(6):
        piece = jnp.concatenate(
            [parts[8 * face_node(face, a, b) :][:8] for a in range(4) for b in range(4)], axis=0
        ).astype(BF16)
        table_ref[:, face * elems : (face + 1) * elems] = piece
    pick = one_hot(iota((6 * elems, 2 * peer), 0) == exports)
    sent = mm(table_ref[...], pick)
    first = iota((8, 2 * peer), 0) < 4
    for m in range(8):
        even = sent[16 * m : 16 * m + 8]
        odd = sent[16 * m + 8 : 16 * m + 16]
        even = even + pltpu.roll(even, 4, 0)
        odd = odd + pltpu.roll(odd, 4, 0)
        both = jnp.where(first, even, odd)
        low_ref[8 * m : 8 * m + 8, :] = both[:, :peer]
        high_ref[8 * m : 8 * m + 8, :] = both[:, peer:]


def live_of(counts_ref, elems):
    return jnp.where(iota((1, elems), 1) < counts_ref[0], 1.0, 0.0)


def prepare(counts, first, source, initial, inverse, lift, lift_time, exports,
            weight, base, table, top, low, high, rows_ref):
    elems = source.shape[2]
    dup = iota((512, 256), 0)
    row_pick = one_hot((dup % 4) * 64 + dup // 8 == iota((512, 256), 1))
    inv_hi, inv_lo = split(inverse[...])
    inv_hi = mm(row_pick, inv_hi).astype(BF16)
    inv_lo = mm(row_pick, inv_lo).astype(BF16)

    def solve(x_hi, x_lo):
        return mm(inv_hi, x_hi) + (mm(inv_hi, x_lo) + mm(inv_lo, x_hi))

    start = initial[...] * jnp.where(first[0] > 0, 1.0, 0.0)
    lt_hi, lt_lo = split(lift_time[...].T)
    st_hi, st_lo = split(start)
    rhs = source[0] + (mm(lt_hi, st_hi) + (mm(lt_hi, st_lo) + mm(lt_lo, st_hi)))
    rows = solve(*split(rhs)) * live_of(counts, elems)
    base[...] = rows
    publish(rows, rows_ref, exports[...], table, top, low, high)

    col = iota((384, 768), 1)
    want = ((col % 4) * 16 + (col // 8) % 16) * 6 + col // 128
    col_pick = one_hot(want == iota((384, 768), 0))
    l_hi, l_lo = split(lift[...])
    l_hi = mm(l_hi, col_pick).astype(BF16)
    l_lo = mm(l_lo, col_pick).astype(BF16)
    w_hi, w_lo = split(solve(l_hi, l_lo))
    weight[0:512, 0:768] = w_hi
    weight[512:1024, 0:768] = w_lo
    t_hi, t_lo = split(solve(jnp.concatenate([lt_hi, lt_hi], 1), jnp.concatenate([lt_lo, lt_lo], 1)))
    weight[0:512, 768:896] = t_hi
    weight[512:1024, 768:896] = t_lo


def gather_local(table, links, out):
    elems = links.shape[1]
    for face in range(6):
        cols = slice(face * elems, (face + 1) * elems)
        pick = one_hot(iota((6 * elems, elems), 0) == links[face : face + 1, :])
        out[:, cols] = mm(table[...], pick).astype(BF16)


def advance(counts, local, from_low, from_high, top_in, weight, base, links, orient, nbr):
    elems = base.shape[1]
    peer = from_low.shape[1]
    first = iota((8, peer), 0) < 4
    sides = []
    for ref in (from_low, from_high):
        slabs = []
        for m in range(8):
            v = ref[8 * m : 8 * m + 8, :]
            r = pltpu.roll(v, 4, 0)
            slabs += [jnp.where(first, v, r), jnp.where(first, r, v)]
        sides.append(halves(jnp.concatenate(slabs, axis=0)).astype(BF16))
    imported = jnp.concatenate(sides, axis=1)
    for face in range(6):
        cols = slice(face * elems, (face + 1) * elems)
        pick = one_hot(iota((2 * peer, elems), 0) + 6 * elems == links[face : face + 1, :])
        got = local[:, cols].astype(F32) + mm(imported, pick)
        turn = jnp.broadcast_to(orient[face : face + 1, :], (8, elems))
        swap = (turn & 4) > 0
        rev_a = (turn & 1) > 0
        rev_b = (turn & 2) > 0
        v = [[got[8 * (a * 4 + b) :][:8] for b in range(4)] for a in range(4)]
        v = [[v[a][b] if a == b else jnp.where(swap, v[b][a], v[a][b]) for b in range(4)] for a in range(4)]
        v = [[jnp.where(rev_a, v[3 - a][b], v[a][b]) for b in range(4)] for a in range(4)]
        v = [[jnp.where(rev_b, v[a][3 - b], v[a][b]) for b in range(4)] for a in range(4)]
        nbr[face * 128 : (face + 1) * 128, :] = jnp.concatenate(sum(v, []), axis=0).astype(BF16)
    t_hi, t_lo = split(top_in[...])
    nbr[768:832, :] = t_hi
    nbr[832:896, :] = t_lo
    x = nbr[...]
    both = mm(weight[0:512, :], x) + mm(weight[512:1024, :], x)
    return (both + base[...]) * live_of(counts, elems)


def step_kernel(counts, local, from_low, from_high, top_in, weight, base, links, orient, exports,
                table, top, low, high, nbr, rows_ref):
    rows = advance(counts, local, from_low, from_high, top_in, weight, base, links, orient, nbr)
    publish(rows, rows_ref, exports[...], table, top, low, high)


def last_kernel(counts, local, from_low, from_high, top_in, weight, base, links, orient,
                out, nbr, rows_ref):
    rows = advance(counts, local, from_low, from_high, top_in, weight, base, links, orient, nbr)
    for c in range(rows_ref.shape[0]):
        rows_ref[c] = rows[:, c * 128 : (c + 1) * 128]
        for t in range(4):
            out[0, t * 64 : (t + 1) * 64, c * 128 : (c + 1) * 128] = rows_ref[c, pl.ds(t, 64, stride=8), :]


def body(source, initial, inverse, lift, lift_time, links, orient, exports, counts):
    elems = links.shape[1]
    peer = exports.shape[0] // 2
    exports = exports.reshape(1, 2 * peer)
    first = (lax.axis_index("slab") == 0).astype(jnp.int32).reshape(1)
    spaces = lax.axis_size("space")
    up = [(i, (i + 1) % spaces) for i in range(spaces)]
    down = [(b, a) for a, b in up]
    later = [(i, i + 1) for i in range(lax.axis_size("slab") - 1)]
    S = pltpu.VMEM
    params = pltpu.CompilerParams(vmem_limit_bytes=24 * 1024 * 1024)
    published = [
        S((128, 6 * elems), BF16),
        S((64, elems), F32),
        S((64, peer), F32),
        S((64, peer), F32),
    ]
    rows_scratch = pltpu.VMEM((elems // 128, 512, 128), F32)
    nbr_scratch = pltpu.VMEM((896, elems), BF16)

    weight, base, table, top, low, high = pl.pallas_call(
        prepare,
        out_shape=[S((1024, 896), BF16), S((512, elems), F32)] + published,
        in_specs=[SMEM, SMEM] + [VMEM] * 6,
        out_specs=[VMEM] * 6,
        scratch_shapes=[rows_scratch],
        compiler_params=params,
        name="prepare",
    )(counts, first, source, initial, inverse, lift, lift_time.T, exports)
    for step in range(1, ITERS):
        from_low = lax.ppermute(high, "space", up)
        from_high = lax.ppermute(low, "space", down)
        top_in = lax.ppermute(top, "slab", later)
        local = pl.pallas_call(
            gather_local,
            out_shape=S((128, 6 * elems), BF16),
            in_specs=[VMEM] * 2,
            out_specs=VMEM,
            compiler_params=params,
            name="gather_local",
        )(table, links)
        from_low, from_high, top_in = (
            pltpu.with_memory_space_constraint(x, pltpu.VMEM) for x in (from_low, from_high, top_in)
        )
        args = (counts, local, from_low, from_high, top_in, weight, base, links, orient)
        if step < ITERS - 1:
            table, top, low, high = pl.pallas_call(
                step_kernel,
                out_shape=published,
                in_specs=[SMEM] + [VMEM] * 9,
                out_specs=[VMEM] * 4,
                scratch_shapes=[nbr_scratch, rows_scratch],
                compiler_params=params,
                name="advance",
            )(*args, exports)
        else:
            out = pl.pallas_call(
                last_kernel,
                out_shape=jax.ShapeDtypeStruct((1, 256, elems), F32),
                in_specs=[SMEM] + [VMEM] * 8,
                out_specs=VMEM,
                scratch_shapes=[nbr_scratch, rows_scratch],
                compiler_params=params,
                name="advance_last",
            )(*args)
    return out


def solution(mesh):
    return jax.shard_map(
        body,
        mesh=mesh,
        in_specs=(
            P("slab", None, "space"),
            P(None, "space"),
            P(),
            P(),
            P(),
            P(None, "space"),
            P(None, "space"),
            P("space"),
            P("space"),
        ),
        out_specs=P("slab", None, "space"),
        check_vma=False,
    )
```

```python
import jax
import jax.numpy as jnp
from jax import lax
from jax.experimental import pallas as pl
from jax.experimental.pallas import tpu as pltpu
from jax.sharding import PartitionSpec as P

ITERS = 6
F32 = jnp.float32
BF16 = jnp.bfloat16

VMEM = pl.BlockSpec(memory_space=pltpu.VMEM)
HBM = pl.BlockSpec(memory_space=pltpu.HBM)
SMEM = pl.BlockSpec(memory_space=pltpu.SMEM)


def mm(a, b):
    return jnp.dot(a, b, preferred_element_type=F32)


def split(x):
    hi = x.astype(BF16)
    return hi, (x - hi.astype(F32)).astype(BF16)


def iota(shape, dim):
    return lax.broadcasted_iota(jnp.int32, shape, dim)


def one_hot(hit):
    return jnp.where(hit, 1.0, 0.0).astype(BF16)


def halves(x):
    hi = x.astype(BF16).astype(F32)
    return jnp.where(iota(x.shape, 0) % 8 < 4, hi, x - hi)


def face_node(face, a, b):
    end = 3 * (face % 2)
    if face < 2:
        return end * 16 + a * 4 + b
    if face < 4:
        return a * 16 + end * 4 + b
    return a * 16 + b * 4 + end


def publish(rows, rows_ref, exports, table_ref, top_ref, low_ref, high_ref):
    elems = rows.shape[1]
    peer = low_ref.shape[1]
    for c in range(rows_ref.shape[0]):
        rows_ref[c] = rows[:, c * 128 : (c + 1) * 128]
        top_ref[:, c * 128 : (c + 1) * 128] = rows_ref[c, pl.ds(3, 64, stride=8), :]
    parts = halves(rows)
    sent = None
    for face in range(6):
        piece = jnp.concatenate(
            [parts[8 * face_node(face, a, b) :][:8] for a in range(4) for b in range(4)], axis=0
        ).astype(BF16)
        table_ref[:, face * elems : (face + 1) * elems] = piece
    pick = one_hot(iota((6 * elems, 2 * peer), 0) == exports)
    sent = mm(table_ref[...], pick)
    first = iota((8, 2 * peer), 0) < 4
    for m in range(8):
        even = sent[16 * m : 16 * m + 8]
        odd = sent[16 * m + 8 : 16 * m + 16]
        even = even + pltpu.roll(even, 4, 0)
        odd = odd + pltpu.roll(odd, 4, 0)
        both = jnp.where(first, even, odd)
        low_ref[8 * m : 8 * m + 8, :] = both[:, :peer]
        high_ref[8 * m : 8 * m + 8, :] = both[:, peer:]


def live_of(counts_ref, elems):
    return jnp.where(iota((1, elems), 1) < counts_ref[0], 1.0, 0.0)


def fetch(sources, targets, sems):
    copies = [pltpu.make_async_copy(a, b, sems.at[i]) for i, (a, b) in enumerate(zip(sources, targets))]
    for copy in copies:
        copy.start()
    for copy in copies:
        copy.wait()


def inverse_parts(inverse):
    dup = iota((512, 256), 0)
    row_pick = one_hot((dup % 4) * 64 + dup // 8 == iota((512, 256), 1))
    inv_hi, inv_lo = split(inverse)
    return mm(row_pick, inv_hi).astype(BF16), mm(row_pick, inv_lo).astype(BF16)


def product(a, b):
    return mm(a[0], b[0]) + (mm(a[0], b[1]) + mm(a[1], b[0]))


def prepare(counts, first, source_hbm, initial_hbm, inverse_hbm, lift_time_hbm, exports_hbm,
            base, table, top, low, high, source, initial, inverse, lift_time, exports, rows_ref, sems):
    fetch(
        (source_hbm, initial_hbm, inverse_hbm, lift_time_hbm, exports_hbm),
        (source, initial, inverse, lift_time, exports),
        sems,
    )
    elems = source.shape[2]
    start = initial[...] * jnp.where(first[0] > 0, 1.0, 0.0)
    rhs = source[0] + product(split(lift_time[...].T), split(start))
    rows = product(inverse_parts(inverse[...]), split(rhs)) * live_of(counts, elems)
    base[...] = rows
    publish(rows, rows_ref, exports[...], table, top, low, high)


def fold_lifts(inverse_hbm, lift_hbm, lift_time_hbm, weight, inverse, lift, lift_time, sems):
    fetch((inverse_hbm, lift_hbm, lift_time_hbm), (inverse, lift, lift_time), sems)
    inv = inverse_parts(inverse[...])
    col = iota((384, 768), 1)
    want = ((col % 4) * 16 + (col // 8) % 16) * 6 + col // 128
    col_pick = one_hot(want == iota((384, 768), 0))
    l_hi, l_lo = split(lift[...])
    l_hi = mm(l_hi, col_pick).astype(BF16)
    l_lo = mm(l_lo, col_pick).astype(BF16)
    w_hi, w_lo = split(product(inv, (l_hi, l_lo)))
    weight[0:512, 0:768] = w_hi
    weight[512:1024, 0:768] = w_lo
    time = lift_time[...].T
    t_hi, t_lo = split(product(inv, split(jnp.concatenate([time, time], 1))))
    weight[0:512, 768:896] = t_hi
    weight[512:1024, 768:896] = t_lo


def gather_local(table, links, out):
    elems = links.shape[1]
    for face in range(6):
        cols = slice(face * elems, (face + 1) * elems)
        pick = one_hot(iota((6 * elems, elems), 0) == links[face : face + 1, :])
        out[:, cols] = mm(table[...], pick).astype(BF16)


def advance(counts, local, from_low, from_high, top_in, weight, base, links, orient, nbr):
    elems = base.shape[1]
    peer = from_low.shape[1]
    first = iota((8, peer), 0) < 4
    sides = []
    for ref in (from_low, from_high):
        slabs = []
        for m in range(8):
            v = ref[8 * m : 8 * m + 8, :]
            r = pltpu.roll(v, 4, 0)
            slabs += [jnp.where(first, v, r), jnp.where(first, r, v)]
        sides.append(halves(jnp.concatenate(slabs, axis=0)).astype(BF16))
    imported = jnp.concatenate(sides, axis=1)
    for face in range(6):
        cols = slice(face * elems, (face + 1) * elems)
        pick = one_hot(iota((2 * peer, elems), 0) + 6 * elems == links[face : face + 1, :])
        got = local[:, cols].astype(F32) + mm(imported, pick)
        turn = jnp.broadcast_to(orient[face : face + 1, :], (8, elems))
        swap = (turn & 4) > 0
        rev_a = (turn & 1) > 0
        rev_b = (turn & 2) > 0
        v = [[got[8 * (a * 4 + b) :][:8] for b in range(4)] for a in range(4)]
        v = [[v[a][b] if a == b else jnp.where(swap, v[b][a], v[a][b]) for b in range(4)] for a in range(4)]
        v = [[jnp.where(rev_a, v[3 - a][b], v[a][b]) for b in range(4)] for a in range(4)]
        v = [[jnp.where(rev_b, v[a][3 - b], v[a][b]) for b in range(4)] for a in range(4)]
        nbr[face * 128 : (face + 1) * 128, :] = jnp.concatenate(sum(v, []), axis=0).astype(BF16)
    t_hi, t_lo = split(top_in[...])
    nbr[768:832, :] = t_hi
    nbr[832:896, :] = t_lo
    x = nbr[...]
    both = mm(weight[0:512, :], x) + mm(weight[512:1024, :], x)
    return (both + base[...]) * live_of(counts, elems)


def step_kernel(counts, local, from_low, from_high, top_in, weight, base, links, orient, exports,
                table, top, low, high, nbr, rows_ref):
    rows = advance(counts, local, from_low, from_high, top_in, weight, base, links, orient, nbr)
    publish(rows, rows_ref, exports[...], table, top, low, high)


def last_kernel(counts, local, from_low, from_high, top_in, weight, base, links, orient,
                out, nbr, rows_ref):
    rows = advance(counts, local, from_low, from_high, top_in, weight, base, links, orient, nbr)
    for c in range(rows_ref.shape[0]):
        rows_ref[c] = rows[:, c * 128 : (c + 1) * 128]
        for t in range(4):
            out[0, t * 64 : (t + 1) * 64, c * 128 : (c + 1) * 128] = rows_ref[c, pl.ds(t, 64, stride=8), :]


def body(source, initial, inverse, lift, lift_time, links, orient, exports, counts):
    elems = links.shape[1]
    peer = exports.shape[0] // 2
    exports = exports.reshape(1, 2 * peer)
    first = (lax.axis_index("slab") == 0).astype(jnp.int32).reshape(1)
    spaces = lax.axis_size("space")
    up = [(i, (i + 1) % spaces) for i in range(spaces)]
    down = [(b, a) for a, b in up]
    later = [(i, i + 1) for i in range(lax.axis_size("slab") - 1)]
    S = pltpu.VMEM
    params = pltpu.CompilerParams(vmem_limit_bytes=24 * 1024 * 1024)
    published = [
        S((128, 6 * elems), BF16),
        S((64, elems), F32),
        S((64, peer), F32),
        S((64, peer), F32),
    ]
    rows_scratch = pltpu.VMEM((elems // 128, 512, 128), F32)
    nbr_scratch = pltpu.VMEM((896, elems), BF16)

    def copied(*arrays):
        return [pltpu.VMEM(x.shape, x.dtype) for x in arrays]

    lift_time = lift_time.T
    source, initial, inverse, lift, lift_time, exports_in = (
        pltpu.with_memory_space_constraint(x, pltpu.HBM)
        for x in (source, initial, inverse, lift, lift_time, exports)
    )
    fetched = (source, initial, inverse, lift_time, exports_in)
    base, table, top, low, high = pl.pallas_call(
        prepare,
        out_shape=[S((512, elems), F32)] + published,
        in_specs=[SMEM, SMEM] + [HBM] * 5,
        out_specs=[VMEM] * 5,
        scratch_shapes=copied(*fetched) + [rows_scratch, pltpu.SemaphoreType.DMA((5,))],
        compiler_params=params,
        name="prepare",
    )(counts, first, *fetched)
    fetched = (inverse, lift, lift_time)
    weight = pl.pallas_call(
        fold_lifts,
        out_shape=S((1024, 896), BF16),
        in_specs=[HBM] * 3,
        out_specs=VMEM,
        scratch_shapes=copied(*fetched) + [pltpu.SemaphoreType.DMA((3,))],
        compiler_params=params,
        name="fold_lifts",
    )(*fetched)
    for step in range(1, ITERS):
        from_low = lax.ppermute(high, "space", up)
        from_high = lax.ppermute(low, "space", down)
        top_in = lax.ppermute(top, "slab", later)
        local = pl.pallas_call(
            gather_local,
            out_shape=S((128, 6 * elems), BF16),
            in_specs=[VMEM] * 2,
            out_specs=VMEM,
            compiler_params=params,
            name="gather_local",
        )(table, links)
        from_low, from_high, top_in = (
            pltpu.with_memory_space_constraint(x, pltpu.VMEM) for x in (from_low, from_high, top_in)
        )
        args = (counts, local, from_low, from_high, top_in, weight, base, links, orient)
        if step < ITERS - 1:
            table, top, low, high = pl.pallas_call(
                step_kernel,
                out_shape=published,
                in_specs=[SMEM] + [VMEM] * 9,
                out_specs=[VMEM] * 4,
                scratch_shapes=[nbr_scratch, rows_scratch],
                compiler_params=params,
                name="advance",
            )(*args, exports)
        else:
            out = pl.pallas_call(
                last_kernel,
                out_shape=jax.ShapeDtypeStruct((1, 256, elems), F32),
                in_specs=[SMEM] + [VMEM] * 8,
                out_specs=VMEM,
                scratch_shapes=[nbr_scratch, rows_scratch],
                compiler_params=params,
                name="advance_last",
            )(*args)
    return out


def solution(mesh):
    return jax.shard_map(
        body,
        mesh=mesh,
        in_specs=(
            P("slab", None, "space"),
            P(None, "space"),
            P(),
            P(),
            P(),
            P(None, "space"),
            P(None, "space"),
            P("space"),
            P("space"),
        ),
        out_specs=P("slab", None, "space"),
        check_vma=False,
    )
```

```python
import jax
import jax.numpy as jnp
from jax import lax
from jax.experimental import pallas as pl
from jax.experimental.pallas import tpu as pltpu
from jax.sharding import PartitionSpec as P

ITERS = 6
F32 = jnp.float32
BF16 = jnp.bfloat16

VMEM = pl.BlockSpec(memory_space=pltpu.VMEM)
HBM = pl.BlockSpec(memory_space=pltpu.HBM)
SMEM = pl.BlockSpec(memory_space=pltpu.SMEM)


def mm(a, b):
    return jnp.dot(a, b, preferred_element_type=F32)


def split(x):
    hi = x.astype(BF16)
    return hi, (x - hi.astype(F32)).astype(BF16)


def iota(shape, dim):
    return lax.broadcasted_iota(jnp.int32, shape, dim)


def one_hot(hit):
    return jnp.where(hit, 1.0, 0.0).astype(BF16)


def halves(x):
    hi = x.astype(BF16).astype(F32)
    return jnp.where(iota(x.shape, 0) % 8 < 4, hi, x - hi)


def face_node(face, a, b):
    end = 3 * (face % 2)
    if face < 2:
        return end * 16 + a * 4 + b
    if face < 4:
        return a * 16 + end * 4 + b
    return a * 16 + b * 4 + end


def publish(rows, rows_ref, exports, table_ref, top_ref, low_ref, high_ref):
    elems = rows.shape[1]
    peer = low_ref.shape[1]
    for c in range(rows_ref.shape[0]):
        rows_ref[c] = rows[:, c * 128 : (c + 1) * 128]
        top_ref[:, c * 128 : (c + 1) * 128] = rows_ref[c, pl.ds(3, 64, stride=8), :]
    parts = halves(rows)
    sent = None
    for face in range(6):
        piece = jnp.concatenate(
            [parts[8 * face_node(face, a, b) :][:8] for a in range(4) for b in range(4)], axis=0
        ).astype(BF16)
        table_ref[:, face * elems : (face + 1) * elems] = piece
    pick = one_hot(iota((6 * elems, 2 * peer), 0) == exports)
    sent = mm(table_ref[...], pick)
    first = iota((8, 2 * peer), 0) < 4
    for m in range(8):
        even = sent[16 * m : 16 * m + 8]
        odd = sent[16 * m + 8 : 16 * m + 16]
        even = even + pltpu.roll(even, 4, 0)
        odd = odd + pltpu.roll(odd, 4, 0)
        both = jnp.where(first, even, odd)
        low_ref[8 * m : 8 * m + 8, :] = both[:, :peer]
        high_ref[8 * m : 8 * m + 8, :] = both[:, peer:]


def live_of(counts_ref, elems):
    return jnp.where(iota((1, elems), 1) < counts_ref[0], 1.0, 0.0)


def fetch(sources, targets, sems):
    copies = [pltpu.make_async_copy(a, b, sems.at[i]) for i, (a, b) in enumerate(zip(sources, targets))]
    for copy in copies:
        copy.start()
    for copy in copies:
        copy.wait()


def inverse_parts(inverse):
    dup = iota((512, 256), 0)
    row_pick = one_hot((dup % 4) * 64 + dup // 8 == iota((512, 256), 1))
    inv_hi, inv_lo = split(inverse)
    return mm(row_pick, inv_hi).astype(BF16), mm(row_pick, inv_lo).astype(BF16)


def product(a, b):
    return mm(a[0], b[0]) + (mm(a[0], b[1]) + mm(a[1], b[0]))


def prepare(counts, first, source_hbm, initial_hbm, inverse_hbm, lift_time_hbm, exports_hbm,
            base, table, top, low, high, source, initial, inverse, lift_time, exports, rows_ref, sems):
    fetch(
        (source_hbm, initial_hbm, inverse_hbm, lift_time_hbm, exports_hbm),
        (source, initial, inverse, lift_time, exports),
        sems,
    )
    elems = source.shape[2]
    start = initial[...] * jnp.where(first[0] > 0, 1.0, 0.0)
    rhs = source[0] + product(split(lift_time[...].T), split(start))
    rows = product(inverse_parts(inverse[...]), split(rhs)) * live_of(counts, elems)
    base[...] = rows
    publish(rows, rows_ref, exports[...], table, top, low, high)


def fold_lifts(inverse_hbm, lift_hbm, lift_time_hbm, weight, inverse, lift, lift_time, sems):
    fetch((inverse_hbm, lift_hbm, lift_time_hbm), (inverse, lift, lift_time), sems)
    inv = inverse_parts(inverse[...])
    col = iota((384, 768), 1)
    want = ((col % 4) * 16 + (col // 8) % 16) * 6 + col // 128
    col_pick = one_hot(want == iota((384, 768), 0))
    l_hi, l_lo = split(lift[...])
    l_hi = mm(l_hi, col_pick).astype(BF16)
    l_lo = mm(l_lo, col_pick).astype(BF16)
    w_hi, w_lo = split(product(inv, (l_hi, l_lo)))
    weight[0:512, 0:768] = w_hi
    weight[512:1024, 0:768] = w_lo
    time = lift_time[...].T
    t_hi, t_lo = split(product(inv, split(jnp.concatenate([time, time], 1))))
    weight[0:512, 768:896] = t_hi
    weight[512:1024, 768:896] = t_lo


def gather_local(table, links, out):
    elems = links.shape[1]
    for face in range(6):
        cols = slice(face * elems, (face + 1) * elems)
        pick = one_hot(iota((6 * elems, elems), 0) == links[face : face + 1, :])
        out[:, cols] = mm(table[...], pick).astype(BF16)


def advance(counts, local, from_low, from_high, top_in, weight, base, links, orient, nbr):
    elems = base.shape[1]
    peer = from_low.shape[1]
    first = iota((8, peer), 0) < 4
    sides = []
    for ref in (from_low, from_high):
        slabs = []
        for m in range(8):
            v = ref[8 * m : 8 * m + 8, :]
            r = pltpu.roll(v, 4, 0)
            slabs += [jnp.where(first, v, r), jnp.where(first, r, v)]
        sides.append(halves(jnp.concatenate(slabs, axis=0)).astype(BF16))
    imported = jnp.concatenate(sides, axis=1)
    for face in range(6):
        cols = slice(face * elems, (face + 1) * elems)
        pick = one_hot(iota((2 * peer, elems), 0) + 6 * elems == links[face : face + 1, :])
        got = local[:, cols].astype(F32) + mm(imported, pick)
        turn = jnp.broadcast_to(orient[face : face + 1, :], (8, elems))
        swap = (turn & 4) > 0
        rev_a = (turn & 1) > 0
        rev_b = (turn & 2) > 0
        v = [[got[8 * (a * 4 + b) :][:8] for b in range(4)] for a in range(4)]
        v = [[v[a][b] if a == b else jnp.where(swap, v[b][a], v[a][b]) for b in range(4)] for a in range(4)]
        v = [[jnp.where(rev_a, v[3 - a][b], v[a][b]) for b in range(4)] for a in range(4)]
        v = [[jnp.where(rev_b, v[a][3 - b], v[a][b]) for b in range(4)] for a in range(4)]
        nbr[face * 128 : (face + 1) * 128, :] = jnp.concatenate(sum(v, []), axis=0).astype(BF16)
    t_hi, t_lo = split(top_in[...])
    nbr[768:832, :] = t_hi
    nbr[832:896, :] = t_lo
    x = nbr[...]
    both = mm(weight[0:512, :], x) + mm(weight[512:1024, :], x)
    return (both + base[...]) * live_of(counts, elems)


def step_kernel(counts, local, from_low, from_high, top_in, weight, base, links, orient, exports,
                table, top, low, high, nbr, rows_ref):
    rows = advance(counts, local, from_low, from_high, top_in, weight, base, links, orient, nbr)
    publish(rows, rows_ref, exports[...], table, top, low, high)


def last_kernel(counts, local, from_low, from_high, top_in, weight, base, links, orient,
                out, nbr, rows_ref):
    rows = advance(counts, local, from_low, from_high, top_in, weight, base, links, orient, nbr)
    for c in range(rows_ref.shape[0]):
        rows_ref[c] = rows[:, c * 128 : (c + 1) * 128]
        for t in range(4):
            out[0, t * 64 : (t + 1) * 64, c * 128 : (c + 1) * 128] = rows_ref[c, pl.ds(t, 64, stride=8), :]


def body(source, initial, inverse, lift, lift_time, links, orient, exports, counts):
    elems = links.shape[1]
    peer = exports.shape[0] // 2
    exports = exports.reshape(1, 2 * peer)
    first = (lax.axis_index("slab") == 0).astype(jnp.int32).reshape(1)
    spaces = lax.axis_size("space")
    up = [(i, (i + 1) % spaces) for i in range(spaces)]
    down = [(b, a) for a, b in up]
    later = [(i, i + 1) for i in range(lax.axis_size("slab") - 1)]
    S = pltpu.VMEM
    params = pltpu.CompilerParams(vmem_limit_bytes=24 * 1024 * 1024)
    published = [
        S((128, 6 * elems), BF16),
        S((64, elems), F32),
        S((64, peer), F32),
        S((64, peer), F32),
    ]
    rows_scratch = pltpu.VMEM((elems // 128, 512, 128), F32)
    nbr_scratch = pltpu.VMEM((896, elems), BF16)

    def copied(*arrays):
        return [pltpu.VMEM(x.shape, x.dtype) for x in arrays]

    lift_time = lift_time.T
    source, initial, inverse, lift, lift_time, exports_in = (
        pltpu.with_memory_space_constraint(x, pltpu.HBM)
        for x in (source, initial, inverse, lift, lift_time, exports)
    )
    fetched = (source, initial, inverse, lift_time, exports_in)
    base, table, top, low, high = pl.pallas_call(
        prepare,
        out_shape=[S((512, elems), F32)] + published,
        in_specs=[SMEM, SMEM] + [HBM] * 5,
        out_specs=[VMEM] * 5,
        scratch_shapes=copied(*fetched) + [rows_scratch, pltpu.SemaphoreType.DMA((5,))],
        compiler_params=params,
        name="prepare",
    )(counts, first, *fetched)
    fetched = (inverse, lift, lift_time)
    weight = pl.pallas_call(
        fold_lifts,
        out_shape=S((1024, 896), BF16),
        in_specs=[HBM] * 3,
        out_specs=VMEM,
        scratch_shapes=copied(*fetched) + [pltpu.SemaphoreType.DMA((3,))],
        compiler_params=params,
        name="fold_lifts",
    )(*fetched)
    for step in range(1, ITERS):
        from_low = lax.ppermute(high, "space", up)
        from_high = lax.ppermute(low, "space", down)
        local = pl.pallas_call(
            gather_local,
            out_shape=S((128, 6 * elems), BF16),
            in_specs=[VMEM] * 2,
            out_specs=VMEM,
            compiler_params=params,
            name="gather_local",
        )(table, links)
        top, local = lax.optimization_barrier((top, local))
        top_in = lax.ppermute(top, "slab", later)
        from_low, from_high, top_in = (
            pltpu.with_memory_space_constraint(x, pltpu.VMEM) for x in (from_low, from_high, top_in)
        )
        args = (counts, local, from_low, from_high, top_in, weight, base, links, orient)
        if step < ITERS - 1:
            table, top, low, high = pl.pallas_call(
                step_kernel,
                out_shape=published,
                in_specs=[SMEM] + [VMEM] * 9,
                out_specs=[VMEM] * 4,
                scratch_shapes=[nbr_scratch, rows_scratch],
                compiler_params=params,
                name="advance",
            )(*args, exports)
        else:
            out = pl.pallas_call(
                last_kernel,
                out_shape=jax.ShapeDtypeStruct((1, 256, elems), F32),
                in_specs=[SMEM] + [VMEM] * 8,
                out_specs=VMEM,
                scratch_shapes=[nbr_scratch, rows_scratch],
                compiler_params=params,
                name="advance_last",
            )(*args)
    return out


def solution(mesh):
    return jax.shard_map(
        body,
        mesh=mesh,
        in_specs=(
            P("slab", None, "space"),
            P(None, "space"),
            P(),
            P(),
            P(),
            P(None, "space"),
            P(None, "space"),
            P("space"),
            P("space"),
        ),
        out_specs=P("slab", None, "space"),
        check_vma=False,
    )
```
